32 devices in a mesh: section: 4 (over y, core), tp: 8 (over z, x).
Axes of the slice: x: 2, y: 2, z: 4, core: 2. Of those that a mesh axis runs over, the one named last changes fastest.
Arguments:
- token_ids: int32 [2, 128], replicated, may hold values from 0 to 65535
- alpha_num: int32 [1], replicated, may hold values from 3 to 7
- embed_table: bfloat16 [65536, 8192], P('section', 'tp'), may hold values from -6 to 6
- norm_gain: float32 [4, 8192], P('section'), may hold values from 0.5 to 1.5
- w_query: bfloat16 [4, 8192, 4096], P('section', None, 'tp'), may hold values from -4 to 4
- w_key: bfloat16 [4, 8192, 512], P('section', None, 'tp'), may hold values from -4 to 4
- w_value: bfloat16 [4, 8192, 512], P('section', None, 'tp'), may hold values from -0.0625 to 0.0625
- w_out: bfloat16 [4, 4096, 8192], P('section', 'tp'), may hold values from -0.09375 to 0.09375
Outputs:
- layer_out: bfloat16 [4, 2, 128, 8192], P('section', None, 'tp')
- scales_in: float32 [4, 8192], P('section')
- scales_out: float32 [4, 4096], P('section', 'tp')
- smoothed_q: bfloat16 [4, 8192, 4096], P('section', None, 'tp')
- smoothed_k: bfloat16 [4, 8192, 512], P('section', None, 'tp')
- smoothed_v: bfloat16 [4, 8192, 512], P('section', None, 'tp')
The draws below stay inside these ranges and needn't reach their ends.
All inputs are finite; a program needn't handle non-finite values.
Results may differ from the reference program's by a relative error of at most 0.028.
Values may be sent and summed in bfloat16 or wider, within the bound.
A program may use at most 128 MiB of HBM per device.

```python
import math
import jax
import jax.numpy as jnp
import numpy as np
from jax import lax

D = 8192
HEADS = 32
KV_HEADS = 4
HEAD_DIM = 128
VOCAB = 65536
SEQ = 128
MICRO = 2
LAYERS = 4
QD = 4096
KVD = 512
N_TP = 8


def draw_w_key(key, part):
    fresh = jax.random.normal(jax.random.fold_in(key, 23), (LAYERS, D, KV_HEADS * HEAD_DIM), jnp.float32)
    return (fresh / math.sqrt(D)).astype(jnp.bfloat16)


def draw_w_query(key, part):
    noise = jax.random.normal(jax.random.fold_in(key, 29), (LAYERS, D, HEADS * HEAD_DIM), jnp.float32) / math.sqrt(D)
    return noise.astype(jnp.bfloat16)


def plant(drawn, rng, least, largest):
    place = [jax.random.randint(jax.random.fold_in(rng, axis), (), 0, length) for axis, length in enumerate(drawn.shape)]
    main_axis = drawn.shape.index(max(drawn.shape))
    next_to = place[:main_axis] + [(place[main_axis] + 1) % drawn.shape[main_axis]] + place[main_axis + 1:]
    return drawn.at[tuple(place)].set(least).at[tuple(next_to)].set(largest)


def shard_levels(rng, shape, split, smallest, largest):
    def one(dim, blocks):
        heights = jax.random.uniform(jax.random.fold_in(jax.random.fold_in(rng, 6), dim), (blocks,), jnp.float32, smallest / len(split), largest / len(split))
        return jnp.repeat(jnp.exp(heights), shape[dim] // blocks).reshape((-1,) + (1,) * (len(shape) - dim - 1))

    gain = one(*split[0])
    for cut in split[1:]:
        gain = gain * one(*cut)
    return gain


def rank_table(amount, slope):
    portions = [(1 << 20) // math.isqrt(standing ** slope) + 1 for standing in range(1, amount + 1)]
    width = 1 + sum(portions) // (1 << 30)
    return np.cumsum(np.array([max(1, weight // width) for weight in portions]))


def ranked(rng, extent, count, skew):
    listing = rank_table(count, skew)
    lot = jax.random.randint(jax.random.fold_in(rng, 1), extent, 0, int(listing[count - 1]))
    rank = jnp.searchsorted(jnp.asarray(listing, jnp.int32), lot, side="right")
    return jax.random.permutation(jax.random.fold_in(rng, 2), count)[rank].astype(jnp.int32)


def centred(rng, shape, width, limit, split=(), held_as=jnp.bfloat16):
    result = jax.random.normal(rng, shape, jnp.float32) * width
    if len(split) > 0:
        result = shard_levels(rng, shape, split, -0.22, 0.18) * result
    return jnp.clip(result, min=-limit, max=limit).astype(held_as)


def setup_inputs(seed: int = 0) -> dict:
    keys = jax.random.split(jax.random.key(seed), 9)
    return {
        "token_ids": plant(ranked(keys[0], (MICRO, SEQ), VOCAB, 2), jax.random.fold_in(keys[0], 3), 0, VOCAB - 1).astype(jnp.int32),
        "alpha_num": jax.random.randint(keys[1], (1,), 3, 8).astype(jnp.int32),
        "embed_table": centred(keys[2], (VOCAB, D), 1.0, 6.0, ((0, 4), (1, 8))),
        "norm_gain": jnp.clip(1.0 + 0.1 * jax.random.normal(keys[3], (LAYERS, D), jnp.float32), 0.5, 1.5),
        "w_query": draw_w_query(jax.random.fold_in(keys[8], 71), 0),
        "w_key": draw_w_key(jax.random.fold_in(keys[8], 71), 0),
        "w_value": centred(keys[6], (LAYERS, D, KVD), D ** -0.5, 0.0625, ((0, 4), (2, 8))),
        "w_out": centred(keys[7], (LAYERS, QD, D), QD ** -0.5, 0.09375, ((0, 4), (1, 8))),
    }


norm_eps = 1e-05
stat_eps = 1e-05
rope_base = 500000.0

def rope_tables(length, head_size):
    halves = head_size // 2
    freqs = jnp.exp(-math.log(rope_base) * 2.0 * jnp.arange(halves, dtype=jnp.float32) / head_size)
    angles = jnp.arange(length, dtype=jnp.float32)[:, None] * freqs[None, :]
    return (jnp.cos(angles), jnp.sin(angles))

def rotate(values, cosine, sine):
    halves = values.shape[-1] // 2
    lower = values[..., :halves]
    upper = values[..., halves:]
    cos_rows = cosine[:, None, :]
    sin_rows = sine[:, None, :]
    return jnp.concatenate([lower * cos_rows - upper * sin_rows, upper * cos_rows + lower * sin_rows], axis=-1)

def smoothing(act_peak, weight_peak, alpha_exp):
    return jnp.exp(alpha_exp * jnp.log(act_peak + stat_eps) - (1.0 - alpha_exp) * jnp.log(weight_peak + stat_eps))

def attention_layer(resid, gain_row, query_w, key_w, value_w, out_w):
    length = resid.shape[0]
    values = resid.astype(jnp.float32)
    square = lax.optimization_barrier(jnp.mean(values * values, axis=1, keepdims=True))
    normed = (values * lax.rsqrt(square + norm_eps) * gain_row[None, :]).astype(jnp.bfloat16)
    query = jnp.dot(normed, query_w, preferred_element_type=jnp.float32)
    key_rows = lax.optimization_barrier(jnp.dot(normed, key_w, preferred_element_type=jnp.float32).astype(jnp.bfloat16))
    value_rows = jnp.dot(normed, value_w, preferred_element_type=jnp.float32).astype(jnp.bfloat16)
    cosine, sine = rope_tables(length, HEAD_DIM)
    query_rot = rotate(query.reshape(length, HEADS, HEAD_DIM), cosine, sine).astype(jnp.bfloat16)
    key_rot = rotate(key_rows.astype(jnp.float32).reshape(length, KV_HEADS, HEAD_DIM), cosine, sine).astype(jnp.bfloat16)
    group_size = HEADS // KV_HEADS
    grouped = query_rot.reshape(length, group_size, KV_HEADS, HEAD_DIM).astype(jnp.float32)
    scores = jnp.einsum('qrgd,kgd->grqk', grouped, key_rot.astype(jnp.float32)) / math.sqrt(HEAD_DIM)
    positions = jnp.arange(length, dtype=jnp.int32)
    causal = positions[:, None] >= positions[None, :]
    scores = jnp.where(causal[None, None], scores, -1e+30)
    probs = jax.nn.softmax(scores, axis=-1).astype(jnp.bfloat16)
    value_heads = value_rows.reshape(length, KV_HEADS, HEAD_DIM).astype(jnp.float32)
    attended = jnp.einsum('grqk,kgd->qrgd', probs.astype(jnp.float32), value_heads)
    attended = attended.reshape(length, HEADS * HEAD_DIM).astype(jnp.bfloat16)
    group_cols = HEADS * HEAD_DIM // N_TP
    head_parts = jnp.einsum('qnc,ncd->nqd', attended.reshape(length, N_TP, group_cols).astype(jnp.float32), out_w.reshape(N_TP, group_cols, D).astype(jnp.float32)).astype(jnp.bfloat16)
    mixed = lax.optimization_barrier(jnp.sum(head_parts.astype(jnp.float32), axis=0))
    output = lax.optimization_barrier((values + mixed).astype(jnp.bfloat16))
    normed_peak = lax.optimization_barrier(jnp.max(jnp.abs(normed), axis=0)).astype(jnp.float32)
    attended_peak = lax.optimization_barrier(jnp.max(jnp.abs(attended), axis=0)).astype(jnp.float32)
    return (output, normed_peak, attended_peak)

def reference(token_ids, alpha_num, embed_table, norm_gain, w_query, w_key, w_value, w_out):
    alpha_exp = alpha_num[0].astype(jnp.float32) / 10.0
    stream = jnp.take(embed_table, token_ids, axis=0)
    outputs = []
    inputs_scales = []
    output_scales = []
    smooth_query = []
    smooth_key = []
    smooth_value = []
    for layer_index in range(LAYERS):

        def advance(carry, resid):
            act_peak, head_peak = carry
            output, normed_peak, attended_peak = attention_layer(resid, norm_gain[layer_index], w_query[layer_index], w_key[layer_index], w_value[layer_index], w_out[layer_index])
            return ((jnp.maximum(act_peak, normed_peak), jnp.maximum(head_peak, attended_peak)), output)
        start_peaks = (jnp.zeros((D,), jnp.float32), jnp.zeros((HEADS * HEAD_DIM,), jnp.float32))
        (act_peak, head_peak), stream = lax.scan(advance, start_peaks, stream)
        outputs.append(stream)
        weight_peak = jnp.maximum(jnp.maximum(lax.optimization_barrier(jnp.max(jnp.abs(w_query[layer_index]), axis=1)), lax.optimization_barrier(jnp.max(jnp.abs(w_key[layer_index]), axis=1))), lax.optimization_barrier(jnp.max(jnp.abs(w_value[layer_index]), axis=1))).astype(jnp.float32)
        out_peak = lax.optimization_barrier(jnp.max(jnp.abs(w_out[layer_index]), axis=1)).astype(jnp.float32)
        scale_in = smoothing(act_peak, weight_peak, alpha_exp)
        scale_out = smoothing(head_peak, out_peak, alpha_exp)
        inputs_scales.append(scale_in)
        output_scales.append(scale_out)
        smooth_query.append((w_query[layer_index].astype(jnp.float32) * scale_in[:, None]).astype(jnp.bfloat16))
        smooth_key.append((w_key[layer_index].astype(jnp.float32) * scale_in[:, None]).astype(jnp.bfloat16))
        smooth_value.append((w_value[layer_index].astype(jnp.float32) * scale_in[:, None]).astype(jnp.bfloat16))
    return (jnp.stack(outputs), jnp.stack(inputs_scales), jnp.stack(output_scales), jnp.stack(smooth_query), jnp.stack(smooth_key), jnp.stack(smooth_value))
```

```python
import functools
import math

import jax
import jax.numpy as jnp
from jax import lax
from jax.experimental import pallas as pl
from jax.experimental.pallas import tpu as pltpu
from jax.sharding import PartitionSpec as P

KV_HEADS = 4
HEAD_DIM = 128


norm_eps = 1e-05
stat_eps = 1e-05
rope_base = 500000.0


def rope_tables(length, head_size):
    halves = head_size // 2
    freqs = jnp.exp(-math.log(rope_base) * 2.0 * jnp.arange(halves, dtype=jnp.float32) / head_size)
    angles = jnp.arange(length, dtype=jnp.float32)[:, None] * freqs[None, :]
    return (jnp.cos(angles), jnp.sin(angles))


def smoothing(act_peak, weight_peak, alpha_exp):
    return jnp.exp(
        alpha_exp * jnp.log(act_peak + stat_eps)
        - (1.0 - alpha_exp) * jnp.log(weight_peak + stat_eps)
    )


MESH = pl.DeviceIdType.MESH
CHUNKS = 2
TILE = 512


def remote(src, dst, send, recv, where):
    return pltpu.make_async_remote_copy(
        src_ref=src, dst_ref=dst, send_sem=send, recv_sem=recv, device_id=where, device_id_type=MESH
    )


def grid_of(count):
    minor = 1
    while (2 * minor) * (2 * minor) <= count and count % (2 * minor) == 0:
        minor *= 2
    return (count // minor, minor)


def layers_kernel(
    sections,
    count,
    embedded,
    gain,
    wq_hbm,
    wkv_hbm,
    wo_hbm,
    cos2,
    sin2,
    wpeak_in,
    out,
    act_out,
    head_out,
    wpeak_out,
    wq,
    wkv,
    wo,
    xin,
    ag,
    acc_q,
    acc_kv,
    kvbuf,
    krot,
    vall,
    att,
    part,
    r1,
    s2,
    r2,
    own,
    wpbuf,
    load_sem,
    xin_r,
    xin_s,
    ag_s,
    ag_f,
    ag_r,
    kv_s,
    kv_r,
    r1_s,
    r1_r,
    s2_s,
    r2_r,
    wp_s,
    wp_r,
):
    major, minor = grid_of(count)
    section = lax.axis_index("section")
    me = lax.axis_index("tp")
    a = me // minor
    b = me % minor
    micros, rows, width = embedded.shape
    length = rows * count
    query_cols = wq.shape[1]
    kv_cols = wkv.shape[1] // 2
    heads_here = query_cols // HEAD_DIM
    per_head = HEAD_DIM // kv_cols
    span = width // CHUNKS
    loads = [
        pltpu.make_async_copy(wq_hbm, wq, load_sem.at[0]),
        pltpu.make_async_copy(wkv_hbm, wkv, load_sem.at[1]),
        pltpu.make_async_copy(wo_hbm, wo, load_sem.at[2]),
    ]
    for load in loads:
        load.start()

    def peer(number):
        return (section, number)

    def col_peer(step):
        return lax.rem(a + step + major, major)

    def row_peer(step):
        return lax.rem(b + step + minor, minor)

    barrier = pltpu.get_barrier_semaphore()
    for step in range(1, count):
        pl.semaphore_signal(
            barrier, inc=1, device_id=peer(lax.rem(me + step, count)), device_id_type=MESH
        )

    @pl.when(section > 0)
    def _():
        pl.semaphore_signal(barrier, inc=1, device_id=(section - 1, me), device_id_type=MESH)

    @pl.when(section < sections - 1)
    def _():
        pl.semaphore_signal(barrier, inc=1, device_id=(section + 1, me), device_id_type=MESH)

    before = (section + sections - 1) // sections
    after = (2 * sections - 2 - section) // sections
    pl.semaphore_wait(barrier, count - 1 + before + after)

    act_out[...] = jnp.zeros_like(act_out)
    head_out[...] = jnp.zeros_like(head_out)
    positions = lax.broadcasted_iota(jnp.int32, (length, length), 0)
    keys_at = lax.broadcasted_iota(jnp.int32, (length, length), 1)
    causal = positions >= keys_at

    def weight_copy(step):
        return remote(
            wpeak_in,
            wpbuf.at[me],
            wp_s.at[step - 1],
            wp_r.at[me],
            peer(lax.rem(me + step, count)),
        )

    def rotated(values):
        turned = pltpu.roll(values, HEAD_DIM // 2, 1)
        return (values * cos2[...] + turned * sin2[...]).astype(jnp.bfloat16)

    def tile_at(index):
        return pl.ds(pl.multiple_of(index * TILE, TILE), TILE)

    def micro_step(m, first):
        @pl.when(section == 0)
        def _():
            xin[m] = embedded[m]

        @pl.when(section > 0)
        def _():
            remote(
                xin.at[m], xin.at[m], xin_s.at[0], xin_r.at[m], (section - 1, me)
            ).wait_recv()

        def square(index, total):
            values = xin[m, :, tile_at(index)].astype(jnp.float32)
            return total + jnp.sum(values * values, axis=1, keepdims=True)

        total = lax.fori_loop(
            0, width // TILE, square, jnp.zeros((rows, 1), jnp.float32), unroll=True
        )
        inverse = lax.rsqrt(total / width + norm_eps)
        for index in range(width // TILE):
            cols = pl.ds(index * TILE, TILE)
            values = xin[m, :, cols].astype(jnp.float32)
            ag[m, me, :, cols] = (values * inverse * gain[:, cols]).astype(jnp.bfloat16)

        def column_copy(step):
            return remote(
                ag.at[m, me],
                ag.at[m, me],
                ag_s.at[step - 1],
                ag_r.at[m, me],
                peer(col_peer(step) * minor + b),
            )

        def row_copy(origin, order, step):
            return remote(
                ag.at[m, origin],
                ag.at[m, origin],
                ag_f.at[order, step - 1],
                ag_r.at[m, origin],
                peer(a * minor + row_peer(step)),
            )

        for step in range(1, major):
            column_copy(step).start()
        for step in range(1, minor):
            row_copy(me, 0, step).start()
        for order in range(1, major):
            origin = col_peer(-order) * minor + b
            row_copy(origin, order, 1).wait_recv()
            for step in range(1, minor):
                row_copy(origin, order, step).start()
        for order in range(major):
            for step in range(1, minor):
                origin = col_peer(-order) * minor + row_peer(step)
                row_copy(origin, order, step).wait_recv()

        @pl.when(first)
        def _():
            for load in loads:
                load.wait()
            for step in range(1, count):
                weight_copy(step).start()

        acc_q[...] = jnp.zeros_like(acc_q)
        acc_kv[...] = jnp.zeros_like(acc_kv)

        @pl.loop(0, width // TILE)
        def _(index):
            cols = tile_at(index)
            if rows % 16 == 0:
                normed = ag[m, :, :, cols].reshape(length, TILE)
            else:
                wide = ag[m, :, :, cols].astype(jnp.float32)
                normed = wide.reshape(length, TILE).astype(jnp.bfloat16)
            acc_q[...] += jnp.dot(normed, wq[cols, :], preferred_element_type=jnp.float32)
            acc_kv[...] += jnp.dot(normed, wkv[cols, :], preferred_element_type=jnp.float32)
            peak = jnp.max(jnp.abs(normed.astype(jnp.float32)), axis=0, keepdims=True)
            act_out[:, cols] = jnp.maximum(act_out[:, cols], peak)

        kvbuf[m, me] = acc_kv[...].astype(jnp.bfloat16)

        def kv_copy(step):
            return remote(
                kvbuf.at[m, me],
                kvbuf.at[m, me],
                kv_s.at[step - 1],
                kv_r.at[m, me],
                peer(lax.rem(me + step, count)),
            )

        for step in range(1, count):
            kv_copy(step).start()
        queries = [
            rotated(acc_q[:, head * HEAD_DIM : (head + 1) * HEAD_DIM])
            for head in range(heads_here)
        ]
        for step in range(1, count):
            origin = lax.rem(me - step + count, count)
            remote(
                kvbuf.at[m, origin],
                kvbuf.at[m, origin],
                kv_s.at[step - 1],
                kv_r.at[m, origin],
                peer(origin),
            ).wait_recv()
        for group in range(KV_HEADS):
            blocks = [
                kvbuf[m, group * per_head + piece].astype(jnp.float32) for piece in range(per_head)
            ]
            key = jnp.concatenate([block[:, :kv_cols] for block in blocks], axis=1)
            value = jnp.concatenate([block[:, kv_cols:] for block in blocks], axis=1)
            krot[group] = rotated(key)
            vall[group] = value.astype(jnp.bfloat16)
        for head in range(heads_here):
            if heads_here % KV_HEADS == 0:
                group = head % KV_HEADS
            else:
                group = lax.rem(me * heads_here + head, KV_HEADS)
            scores = lax.dot_general(
                queries[head],
                krot[group],
                (((1,), (1,)), ((), ())),
                preferred_element_type=jnp.float32,
            ) / math.sqrt(HEAD_DIM)
            scores = jnp.where(causal, scores, -1e30)
            weights = jnp.exp(scores - jnp.max(scores, axis=1, keepdims=True))
            probs = (weights / jnp.sum(weights, axis=1, keepdims=True)).astype(jnp.bfloat16)
            mixed = jnp.dot(probs, vall[group], preferred_element_type=jnp.float32)
            mixed = mixed.astype(jnp.bfloat16)
            cols = pl.ds(head * HEAD_DIM, HEAD_DIM)
            att[:, cols] = mixed
            peak = jnp.max(jnp.abs(mixed.astype(jnp.float32)), axis=0, keepdims=True)
            head_out[:, cols] = jnp.maximum(head_out[:, cols], peak)

        orders = list(range(1, major)) + [0]

        def first_copy(chunk, step, order):
            other_b = row_peer(step)
            other_a = col_peer(order)
            return remote(
                part.at[chunk, other_b, other_a],
                r1.at[m, chunk, b, other_a],
                r1_s.at[chunk, step - 1, order],
                r1_r.at[m, chunk, b, other_a],
                peer(a * minor + other_b),
            )

        def second_copy(chunk, order):
            return remote(
                s2.at[chunk, order - 1],
                r2.at[m, chunk, a],
                s2_s.at[chunk, order - 1],
                r2_r.at[m, chunk, a],
                peer(col_peer(order) * minor + b),
            )

        for chunk in range(CHUNKS):

            @pl.loop(0, span // TILE)
            def _(index):
                cols = tile_at(index)
                source = tile_at(index + chunk * (span // TILE))
                product = jnp.dot(att[...], wo[:, source], preferred_element_type=jnp.float32)
                for i in range(major):
                    for j in range(minor):
                        top = (i * minor + j) * rows
                        part[chunk, j, i, :, cols] = product[top : top + rows].astype(jnp.bfloat16)

            for order in orders:
                for step in range(1, minor):
                    first_copy(chunk, step, order).start()
        for chunk in range(CHUNKS):
            for order in orders:
                other_a = col_peer(order)
                for step in range(1, minor):
                    origin = row_peer(step)
                    remote(
                        r1.at[m, chunk, origin, other_a],
                        r1.at[m, chunk, origin, other_a],
                        r1_s.at[chunk, step - 1, order],
                        r1_r.at[m, chunk, origin, other_a],
                        peer(a * minor + origin),
                    ).wait_recv()
                for index in range(span // TILE):
                    cols = pl.ds(index * TILE, TILE)
                    total = part[chunk, b, other_a, :, cols].astype(jnp.float32)
                    for step in range(1, minor):
                        total += r1[m, chunk, row_peer(step), other_a, :, cols].astype(jnp.float32)
                    if order == 0:
                        own[chunk, :, cols] = total
                    else:
                        s2[chunk, order - 1, :, cols] = total.astype(jnp.bfloat16)
                if order != 0:
                    second_copy(chunk, order).start()
        for chunk in range(CHUNKS):
            for order in range(1, major):
                origin = col_peer(-order)
                remote(
                    r2.at[m, chunk, origin],
                    r2.at[m, chunk, origin],
                    s2_s.at[chunk, order - 1],
                    r2_r.at[m, chunk, origin],
                    peer(origin * minor + b),
                ).wait_recv()
            for index in range(span // TILE):
                cols = pl.ds(index * TILE, TILE)
                full = pl.ds(chunk * span + index * TILE, TILE)
                total = own[chunk, :, cols]
                for order in range(1, major):
                    total += r2[m, chunk, col_peer(-order), :, cols].astype(jnp.float32)
                out[m, :, full] = (xin[m, :, full].astype(jnp.float32) + total).astype(jnp.bfloat16)

        def onward():
            return remote(
                out.at[m], xin.at[m], xin_s.at[0], xin_r.at[m], (section + 1, me)
            )

        @pl.when(section < sections - 1)
        def _():
            onward().start()

        for step in range(1, major):
            column_copy(step).wait_send()
        for order in range(major):
            for step in range(1, minor):
                row_copy(col_peer(-order) * minor + b, order, step).wait_send()
        for step in range(1, count):
            kv_copy(step).wait_send()
        for chunk in range(CHUNKS):
            for order in orders:
                for step in range(1, minor):
                    first_copy(chunk, step, order).wait_send()
                if order != 0:
                    second_copy(chunk, order).wait_send()

        @pl.when(section < sections - 1)
        def _():
            onward().wait_send()

    @pl.loop(0, micros)
    def _(m):
        micro_step(m, m == 0)

    peak = wpeak_in[...]
    for step in range(1, count):
        origin = lax.rem(me + step, count)
        remote(
            wpeak_in, wpbuf.at[origin], wp_s.at[step - 1], wp_r.at[origin], peer(origin)
        ).wait_recv()
        peak = jnp.maximum(peak, wpbuf[origin])
    wpeak_out[...] = peak
    for step in range(1, count):
        weight_copy(step).wait_send()


def run_layers(sections, count, embedded, gain, wq, wkv, wo, cos2, sin2, wpeak):
    major, minor = grid_of(count)
    micros, rows, width = embedded.shape
    length = rows * count
    query_cols = wq.shape[1]
    kv_two = wkv.shape[1]
    span = width // CHUNKS
    bf16, f32 = jnp.bfloat16, jnp.float32
    vmem = pl.BlockSpec(memory_space=pltpu.VMEM)
    anywhere = pl.BlockSpec(memory_space=pl.ANY)
    dma = pltpu.SemaphoreType.DMA
    return pl.pallas_call(
        functools.partial(layers_kernel, sections, count),
        out_shape=(
            jax.ShapeDtypeStruct((micros, rows, width), bf16),
            jax.ShapeDtypeStruct((1, width), f32),
            jax.ShapeDtypeStruct((1, query_cols), f32),
            jax.ShapeDtypeStruct(wpeak.shape, f32),
        ),
        in_specs=[vmem, vmem, anywhere, anywhere, anywhere, vmem, vmem, vmem],
        out_specs=(vmem, vmem, vmem, vmem),
        scratch_shapes=[
            pltpu.VMEM(wq.shape, bf16),
            pltpu.VMEM(wkv.shape, bf16),
            pltpu.VMEM(wo.shape, bf16),
            pltpu.VMEM((micros, rows, width), bf16),
            pltpu.VMEM((micros, count, rows, width), bf16),
            pltpu.VMEM((length, query_cols), f32),
            pltpu.VMEM((length, kv_two), f32),
            pltpu.VMEM((micros, count, length, kv_two), bf16),
            pltpu.VMEM((KV_HEADS, length, HEAD_DIM), bf16),
            pltpu.VMEM((KV_HEADS, length, HEAD_DIM), bf16),
            pltpu.VMEM((length, query_cols), bf16),
            pltpu.VMEM((CHUNKS, minor, major, rows, span), bf16),
            pltpu.VMEM((micros, CHUNKS, minor, major, rows, span), bf16),
            pltpu.VMEM((CHUNKS, major - 1, rows, span), bf16),
            pltpu.VMEM((micros, CHUNKS, major, rows, span), bf16),
            pltpu.VMEM((CHUNKS, rows, span), f32),
            pltpu.VMEM((count,) + wpeak.shape, f32),
            dma((3,)),
            dma((micros,)),
            dma((1,)),
            dma((major - 1,)),
            dma((major, minor - 1)),
            dma((micros, count)),
            dma((count - 1,)),
            dma((micros, count)),
            dma((CHUNKS, minor - 1, major)),
            dma((micros, CHUNKS, minor, major)),
            dma((CHUNKS, major - 1)),
            dma((micros, CHUNKS, major)),
            dma((count - 1,)),
            dma((count,)),
        ],
        compiler_params=pltpu.CompilerParams(
            collective_id=0, has_side_effects=True, vmem_limit_bytes=60 * 1024 * 1024
        ),
        name="layers",
    )(embedded, gain, wq, wkv, wo, cos2, sin2, wpeak)


def shards(token_ids, alpha_num, embed_table, norm_gain, w_query, w_key, w_value, w_out):
    tp_count = lax.axis_size("tp")
    section_count = lax.axis_size("section")
    section_index = lax.axis_index("section")
    length = token_ids.shape[1]
    vocab_rows = embed_table.shape[0]
    local_ids = token_ids - section_index * vocab_rows
    inside = (local_ids >= 0) & (local_ids < vocab_rows)
    picked = jnp.take(embed_table, jnp.clip(local_ids, 0, vocab_rows - 1), axis=0)
    picked = jnp.where(inside[:, :, None], picked, jnp.zeros_like(picked))
    summed = lax.psum(picked, "section")
    embedded = lax.all_to_all(summed, "tp", split_axis=1, concat_axis=2, tiled=True)
    w_query, w_key, w_value, w_out = w_query[0], w_key[0], w_value[0], w_out[0]
    w_kv = jnp.concatenate([w_key, w_value], axis=1)
    weight_local = jnp.maximum(
        jnp.max(jnp.abs(w_query), axis=1), jnp.max(jnp.abs(w_kv), axis=1)
    ).astype(jnp.float32)
    out_peak = jnp.max(jnp.abs(w_out), axis=1).astype(jnp.float32)
    cosine, sine = rope_tables(length, HEAD_DIM)
    cos2 = jnp.concatenate([cosine, cosine], axis=1)
    sin2 = jnp.concatenate([-sine, sine], axis=1)
    stored, act_peak, head_peak, weight_peak = run_layers(
        section_count,
        tp_count,
        embedded,
        norm_gain,
        w_query,
        w_kv,
        w_out,
        cos2,
        sin2,
        weight_local.reshape(-1, 128),
    )
    alpha_exp = alpha_num[0].astype(jnp.float32) / 10.0
    scale_in = smoothing(act_peak[0], weight_peak.reshape(-1), alpha_exp)
    scale_out = smoothing(head_peak[0], out_peak, alpha_exp)

    def smoothed(weights):
        return (weights.astype(jnp.float32) * scale_in[:, None]).astype(jnp.bfloat16)

    return (
        stored[None],
        scale_in[None],
        scale_out[None],
        smoothed(w_query)[None],
        smoothed(w_key)[None],
        smoothed(w_value)[None],
    )


def solution(mesh):
    return jax.shard_map(
        shards,
        mesh=mesh,
        in_specs=(
            P(),
            P(),
            P("section", "tp"),
            P("section", None),
            P("section", None, "tp"),
            P("section", None, "tp"),
            P("section", None, "tp"),
            P("section", "tp", None),
        ),
        out_specs=(
            P("section", None, "tp", None),
            P("section", None),
            P("section", "tp"),
            P("section", None, "tp"),
            P("section", None, "tp"),
            P("section", None, "tp"),
        ),
        check_vma=False,
    )
```
